32 devices in a mesh: range: 16 (over z, x, core), dop: 2 (over y).
Axes of the slice: x: 2, y: 2, z: 4, core: 2. Of those that a mesh axis runs over, the one named last changes fastest.
Arguments:
- echoes: float32 [2, 128, 16, 8192], P(None, None, None, ('range', 'dop')), may hold values from -200 to 200
- triplet: int32 [128, 3], replicated, may hold values from 0 to 127, as said below
- bin_taper: float32 [128, 3], replicated, may hold values from 0.2 to 1
- phases: float32 [16], replicated, may hold values from -3.140625 to 3.140625
- excluded: int32 [128, 512], P('dop', 'range'), may hold values 0 or 1
- guard_len: int32 [128], P('dop'), may hold values from 1 to 4, as said below
- train_len: int32 [128], P('dop'), may hold values from 32 to 64, as said below
Outputs:
- cfar_ratio: float32 [128, 8192], P('dop', 'range')
The draws below stay inside these ranges and needn't reach their ends.
Inputs may be any that keep to these rules, and one draw needn't show every extreme that they name: `triplet`: row b holds a bin below b, b itself, and a bin above b, each within 2 of b counted cyclically over 128 bins. `guard_len`: some bin has exactly 4. `train_len`: some bin has exactly 64.
All inputs are finite; a program needn't handle non-finite values. No bound on the sum of `excluded` on one device may be relied on, other than what follows from the above.
Results may differ from the reference program's by a relative error of at most 0.0003.
Values sent between devices are 32-bit elements; how exact they have to be, the bound alone decides.
A program may use at most 64 MiB of HBM per device.

```python
import math
import jax
import jax.numpy as jnp
from jax import lax

CH = 16
BINS = 128
SLOTS = 3
RANGE = 8192
BLOCK = 16
NBLK = 512
GUARD_MAX = 4
TRAIN_MAX = 64


def draw_echoes(key, part):
    keys = jax.random.split(jax.random.fold_in(key, 7), 5)
    spread = 0.6 / math.sqrt(CH)
    mix_real = jnp.eye(CH, dtype=jnp.float32)[None, :, :] + spread * jax.random.truncated_normal(keys[0], -3.0, 3.0, (BINS, CH, CH), jnp.float32)
    mix_imag = spread * jax.random.truncated_normal(keys[1], -3.0, 3.0, (BINS, CH, CH), jnp.float32)
    noise_real = jax.random.truncated_normal(keys[2], -4.0, 4.0, (BINS, CH, RANGE), jnp.float32)
    noise_imag = jax.random.truncated_normal(keys[3], -4.0, 4.0, (BINS, CH, RANGE), jnp.float32)
    level = jnp.exp(jax.random.uniform(keys[4], (BINS, RANGE), jnp.float32, math.log(0.3), math.log(3.0)))
    amplitude = jnp.sqrt(level)[:, None, :]
    highest = lax.Precision.HIGHEST
    real_out = (jnp.einsum('bij,bjr->bir', mix_real, noise_real, precision=highest) - jnp.einsum('bij,bjr->bir', mix_imag, noise_imag, precision=highest)) * amplitude
    imag_out = (jnp.einsum('bij,bjr->bir', mix_real, noise_imag, precision=highest) + jnp.einsum('bij,bjr->bir', mix_imag, noise_real, precision=highest)) * amplitude
    return jnp.stack([real_out, imag_out]).astype(jnp.float32)


def draw_triplet(key, part):
    first_key, second_key = jax.random.split(jax.random.fold_in(key, 11))
    centre = jnp.arange(BINS, dtype=jnp.int32)
    low_bin = (centre - jax.random.randint(first_key, (BINS,), 1, 3, jnp.int32)) % BINS
    high_bin = (centre + jax.random.randint(second_key, (BINS,), 1, 3, jnp.int32)) % BINS
    return jnp.stack([low_bin, centre, high_bin], axis=1).astype(jnp.int32)


def draw_guard_len(key, part):
    first_key, second_key = jax.random.split(jax.random.fold_in(key, 13))
    values = jax.random.randint(first_key, (BINS,), 1, GUARD_MAX + 1, jnp.int32)
    chosen = jax.random.randint(second_key, (), 0, BINS, jnp.int32)
    return values.at[chosen].set(GUARD_MAX).astype(jnp.int32)


def draw_train_len(key, part):
    first_key, second_key = jax.random.split(jax.random.fold_in(key, 17))
    values = jax.random.randint(first_key, (BINS,), TRAIN_MAX // 2, TRAIN_MAX + 1, jnp.int32)
    chosen = jax.random.randint(second_key, (), 0, BINS, jnp.int32)
    return values.at[chosen].set(TRAIN_MAX).astype(jnp.int32)


def plant(array, rng, least, top_value):
    place = [jax.random.randint(jax.random.fold_in(rng, axis), (), 0, length) for axis, length in enumerate(array.shape)]
    main_axis = array.shape.index(max(array.shape))
    next_to = place[:main_axis] + [(place[main_axis] + 1) % array.shape[main_axis]] + place[main_axis + 1:]
    return array.at[tuple(place)].set(least).at[tuple(next_to)].set(top_value)


def setup_inputs(seed: int = 0) -> dict:
    key_list = jax.random.split(jax.random.key(seed), 8)
    echoes = draw_echoes(jax.random.fold_in(key_list[7], 71), 0)
    triplet = draw_triplet(jax.random.fold_in(key_list[7], 71), 0)
    bin_taper = jnp.clip(jax.random.uniform(key_list[2], (BINS, SLOTS), jnp.float32, 0.2, 1.0), 0.2, 1.0)
    phases = jnp.clip(jax.random.uniform(key_list[3], (CH,), jnp.float32, -3.140625, 3.140625), -3.140625, 3.140625)
    excluded = plant((jax.random.randint(key_list[4], (BINS, NBLK), 0, 4) < 1).astype(jnp.int32), jax.random.fold_in(key_list[4], 1), 0, 1)
    guard_len = draw_guard_len(jax.random.fold_in(key_list[7], 71), 0)
    train_len = draw_train_len(jax.random.fold_in(key_list[7], 71), 0)
    return {"echoes": echoes, "triplet": triplet, "bin_taper": bin_taper, "phases": phases, "excluded": excluded, "guard_len": guard_len, "train_len": train_len}


full_precision = lax.Precision.HIGHEST
epsilon = 1e-06

def gram_blocks(snapshot, kept_mask):
    snap_real = snapshot[0]
    snap_imag = snapshot[1]
    kept_real = snap_real * kept_mask[:, None, :]
    kept_imag = snap_imag * kept_mask[:, None, :]
    cov_real = jnp.einsum('bir,bjr->bij', kept_real, snap_real, precision=full_precision) + jnp.einsum('bir,bjr->bij', kept_imag, snap_imag, precision=full_precision)
    cov_imag = jnp.einsum('bir,bjr->bij', kept_imag, snap_real, precision=full_precision) - jnp.einsum('bir,bjr->bij', kept_real, snap_imag, precision=full_precision)
    bin_count = snapshot.shape[1]
    space_time = snapshot.shape[2]
    return jnp.concatenate([cov_real, cov_imag], axis=1).reshape(bin_count, 2 * space_time * space_time)

def solve_system(gram_term, taper_rows, phases, total_range):
    bin_count = gram_term.shape[0]
    space_time = taper_rows.shape[1] * phases.shape[0]
    blocks = gram_term.reshape(bin_count, 2, space_time, space_time)
    real_part = blocks[:, 0]
    imag_part = blocks[:, 1]
    system = jnp.concatenate([jnp.concatenate([real_part, -imag_part], axis=2), jnp.concatenate([imag_part, real_part], axis=2)], axis=1) / total_range
    cosines = (taper_rows[:, :, None] * jnp.cos(phases)[None, None, :]).reshape(bin_count, space_time)
    sines = (taper_rows[:, :, None] * jnp.sin(phases)[None, None, :]).reshape(bin_count, space_time)
    right_side = jnp.concatenate([cosines, sines], axis=1)[:, :, None]
    factor = jnp.linalg.cholesky(system)
    halfway = lax.linalg.triangular_solve(factor, right_side, left_side=True, lower=True)
    solved = lax.linalg.triangular_solve(factor, halfway, left_side=True, lower=True, transpose_a=True)
    return solved[:, :, 0]

def apply_weights(snapshot, weights):
    space_time = snapshot.shape[2]
    weight_real = weights[:, :space_time]
    weight_imag = weights[:, space_time:]
    real_out = jnp.einsum('bi,bir->br', weight_real, snapshot[0], precision=full_precision) + jnp.einsum('bi,bir->br', weight_imag, snapshot[1], precision=full_precision)
    imag_out = jnp.einsum('bi,bir->br', weight_real, snapshot[1], precision=full_precision) - jnp.einsum('bi,bir->br', weight_imag, snapshot[0], precision=full_precision)
    return real_out * real_out + imag_out * imag_out

def detect(power_map, padded, guard_len, train_len, gate_start, total_range, reach_len):
    bin_count = power_map.shape[0]
    cell_total = power_map.shape[1]
    prefix = jnp.concatenate([jnp.zeros((bin_count, 1), padded.dtype), jnp.cumsum(padded, axis=1)], axis=1)
    cell_ids = jnp.arange(cell_total, dtype=jnp.int32)[None, :]
    guard_col = guard_len[:, None].astype(jnp.int32)
    train_col = train_len[:, None].astype(jnp.int32)
    padded_at = cell_ids + reach_len
    left_sum = jnp.take_along_axis(prefix, padded_at - guard_col, axis=1) - jnp.take_along_axis(prefix, padded_at - guard_col - train_col, axis=1)
    right_sum = jnp.take_along_axis(prefix, padded_at + guard_col + train_col + 1, axis=1) - jnp.take_along_axis(prefix, padded_at + guard_col + 1, axis=1)
    position = gate_start + cell_ids
    left_count = jnp.maximum(jnp.minimum(position - guard_col - 1, total_range - 1) - jnp.maximum(position - guard_col - train_col, 0) + 1, 0)
    right_count = jnp.maximum(jnp.minimum(position + guard_col + train_col, total_range - 1) - jnp.maximum(position + guard_col + 1, 0) + 1, 0)
    noise_level = (left_sum + right_sum) / (left_count + right_count).astype(jnp.float32)
    return power_map / (noise_level + epsilon)

def reference(echoes, triplet, bin_taper, phases, excluded, guard_len, train_len):
    total_range = echoes.shape[3]
    space_time = SLOTS * CH
    kept_all = (1 - jnp.repeat(excluded, BLOCK, axis=1)).astype(jnp.float32)

    def one_bin(bin_index):
        bin_rows = lax.dynamic_slice_in_dim(triplet, bin_index, 1, 0).reshape(-1)
        snapshot = jnp.take(echoes, bin_rows, axis=1).reshape(2, 1, space_time, total_range)
        kept_mask = lax.dynamic_slice_in_dim(kept_all, bin_index, 1, 0)
        gram_term = gram_blocks(snapshot, kept_mask)
        taper_rows = lax.dynamic_slice_in_dim(bin_taper, bin_index, 1, 0)
        weights = solve_system(gram_term, taper_rows, phases, total_range)
        return apply_weights(snapshot, weights)[0]
    power_map = lax.map(one_bin, jnp.arange(BINS, dtype=jnp.int32))
    reach_len = GUARD_MAX + TRAIN_MAX
    padded = jnp.pad(power_map, ((0, 0), (reach_len, reach_len)))
    return detect(power_map, padded, guard_len, train_len, 0, total_range, reach_len)
```

```python
import functools

import jax
import jax.numpy as jnp
from jax import lax
from jax.experimental import pallas as pl
from jax.experimental.pallas import tpu as pltpu
from jax.sharding import PartitionSpec as P

BLOCK = 16
GUARD_MAX = 4
TRAIN_MAX = 64
LANES = 128
epsilon = 1e-06

MESH = pl.DeviceIdType.MESH
VMEM = pl.BlockSpec(memory_space=pltpu.VMEM)
SMEM = pl.BlockSpec(memory_space=pltpu.SMEM)
VMEM_LIMIT = 60 * 1024 * 1024


def grid_sizes(range_count, dop_count):
    core = 2 if range_count % 2 == 0 else 1
    rest = range_count // core
    near = 1
    while near * near * 4 <= rest and rest % (near * 2) == 0:
        near *= 2
    return core, dop_count, near, rest // near


def place_of(sizes, index):
    core, dops, near, far = sizes
    c = index // (dops * near * far)
    y = (index // (near * far)) % dops
    x = (index // far) % near
    z = index % far
    return ((z * near + x) * core + c, y)


def my_parts(sizes):
    core, _, near, _ = sizes
    r = lax.axis_index("range")
    return r % core, lax.axis_index("dop"), (r // core) % near, r // (core * near)


def chunk_index(sizes, parts):
    core, dops, near, far = sizes
    c, y, x, z = parts
    return ((c * dops + y) * near + x) * far + z


def greet(devices):
    barrier = pltpu.get_barrier_semaphore()
    for device in devices:
        pl.semaphore_signal(barrier, inc=1, device_id=device, device_id_type=MESH)
    pl.semaphore_wait(barrier, len(devices))


def mask_kernel(dops, excl_ref, out_ref, send_sems, recv_sems, local_sem):
    r = lax.axis_index("range")
    y = lax.axis_index("dop")
    greet([(r, (y + k) % dops) for k in range(1, dops)])
    copies = []
    for k in range(1, dops):
        copies.append(
            pltpu.make_async_remote_copy(
                src_ref=excl_ref,
                dst_ref=out_ref.at[y],
                send_sem=send_sems.at[k - 1],
                recv_sem=recv_sems.at[k - 1],
                device_id=(r, (y + k) % dops),
                device_id_type=MESH,
            )
        )
        copies[-1].start()
    own = pltpu.make_async_copy(excl_ref, out_ref.at[y], local_sem)
    own.start()
    own.wait()
    for copy in copies:
        copy.wait()


def gather_mask(excluded, dops):
    bins, blocks = excluded.shape
    if dops == 1:
        return excluded
    gathered = pl.pallas_call(
        functools.partial(mask_kernel, dops),
        out_shape=jax.ShapeDtypeStruct((dops, bins, blocks), jnp.int32),
        in_specs=[VMEM],
        out_specs=VMEM,
        scratch_shapes=[
            pltpu.SemaphoreType.DMA((dops - 1,)),
            pltpu.SemaphoreType.DMA((dops - 1,)),
            pltpu.SemaphoreType.DMA,
        ],
        compiler_params=pltpu.CompilerParams(collective_id=0, has_side_effects=True),
    )(excluded)
    return gathered.reshape(dops * bins, blocks)


def gram_kernel(trip_ref, echo_ref, excl_ref, out_ref, kept_ref):
    slots = trip_ref.shape[1]
    chans, gates = echo_ref.shape[2:]
    span = slots * chans
    blocks = excl_ref.shape[1]
    first = lax.axis_index("dop") * (gates // BLOCK)
    block_ids = lax.broadcasted_iota(jnp.int32, (blocks, gates), 0)
    gate_blocks = lax.broadcasted_iota(jnp.int32, (blocks, gates), 1) // BLOCK + first
    spread = jnp.where(block_ids == gate_blocks, 1.0, 0.0).astype(jnp.bfloat16)
    kept_ref[...] = 1.0 - jnp.dot(
        excl_ref[...].astype(jnp.float32).astype(jnp.bfloat16),
        spread,
        preferred_element_type=jnp.float32,
    )
    rows = lax.broadcasted_iota(jnp.int32, (span, LANES), 0)
    lanes = lax.broadcasted_iota(jnp.int32, (span, LANES), 1)
    upper_even = rows <= lanes
    upper_odd = rows <= lanes - span
    is_even = lanes < span
    filler = jnp.zeros((LANES - 2 * span, 8 * gates), jnp.bfloat16)

    def split(values):
        high = values.astype(jnp.bfloat16)
        return high, (values - high.astype(jnp.float32)).astype(jnp.bfloat16)

    def pair_step(pair, carry):
        lefts = []
        rights = []
        for s in range(2):
            b = 2 * pair + s
            u = jnp.concatenate([echo_ref[0, trip_ref[b, t]] for t in range(slots)], axis=0)
            v = jnp.concatenate([echo_ref[1, trip_ref[b, t]] for t in range(slots)], axis=0)
            kept = kept_ref[pl.ds(b, 1), :].astype(jnp.bfloat16)
            uh, ul = split(u)
            vh, vl = split(v)
            uhm, ulm, vhm, vlm = uh * kept, ul * kept, vh * kept, vl * kept
            rights.append(jnp.concatenate([uh, vh, uh, vh, ul, vl, ul, vl], axis=1))
            lefts.append(jnp.concatenate([uhm, vhm, ulm, vlm] * 2, axis=1))
            lefts.append(jnp.concatenate([vhm, -uhm, vlm, -ulm] * 2, axis=1))
        left = jnp.concatenate(lefts, axis=0)
        right = jnp.concatenate(rights + [filler], axis=0)
        product = lax.dot_general(
            left, right, (((1,), (1,)), ((), ())), preferred_element_type=jnp.float32
        )
        even = jnp.where(upper_even, product[:span], product[span : 2 * span])
        odd = jnp.where(upper_odd, product[2 * span : 3 * span], product[3 * span :])
        out_ref[pair] = jnp.where(is_even, even, odd)
        return carry

    lax.fori_loop(0, out_ref.shape[0], pair_step, 0)


def gram(triplet, echoes, excl_all):
    bins, slots = triplet.shape
    chans, gates = echoes.shape[2:]
    return pl.pallas_call(
        gram_kernel,
        out_shape=jax.ShapeDtypeStruct((bins // 2, slots * chans, LANES), jnp.float32),
        in_specs=[SMEM, VMEM, VMEM],
        out_specs=VMEM,
        scratch_shapes=[pltpu.VMEM((bins, gates), jnp.float32)],
        compiler_params=pltpu.CompilerParams(vmem_limit_bytes=VMEM_LIMIT),
    )(triplet, echoes, excl_all)


def reduce_plan(sizes, total_rows, span):
    count = sizes[0] * sizes[1] * sizes[2] * sizes[3]
    split_core = (total_rows // span) % count == 0
    plan = []
    rows = total_rows
    for axis, group in enumerate(sizes):
        if group == 1:
            continue
        after = rows if axis == 0 and not split_core else rows // group
        plan.append((axis, group, rows, after))
        rows = after
    return plan, rows


def reduce_kernel(sizes, plan, part_ref, out_ref, *scratch):
    phases = len(plan)
    recv_bufs = scratch[:phases]
    sums = scratch[phases : 2 * phases - 1]
    send_sems, recv_sems = scratch[2 * phases - 1 :]
    parts = my_parts(sizes)

    def peer(axis, group, k):
        moved = list(parts)
        moved[axis] = (parts[axis] + k) % group
        return moved[axis], place_of(sizes, chunk_index(sizes, moved))

    greet([peer(axis, group, k)[1] for axis, group, _, _ in plan for k in range(1, group)])
    current = part_ref
    sem = 0
    for phase, (axis, group, before, after) in enumerate(plan):
        whole = before == after
        copies = []
        for k in range(1, group):
            where, device = peer(axis, group, k)
            start = 0 if whole else pl.multiple_of(where * after, 8)
            copies.append(
                pltpu.make_async_remote_copy(
                    src_ref=current.at[pl.ds(start, after)],
                    dst_ref=recv_bufs[phase].at[k - 1],
                    send_sem=send_sems.at[sem],
                    recv_sem=recv_sems.at[sem],
                    device_id=device,
                    device_id_type=MESH,
                )
            )
            copies[-1].start()
            sem += 1
        own = 0 if whole else pl.multiple_of(parts[axis] * after, 8)
        for copy in copies:
            copy.wait()
        total = current[pl.ds(own, after), :]
        for k in range(1, group):
            total = total + recv_bufs[phase][k - 1]
        if phase == phases - 1:
            out_ref[...] = total
        else:
            sums[phase][...] = total
            current = sums[phase]


def reduce_grams(partial, sizes, span):
    total_rows = partial.shape[0]
    plan, rows = reduce_plan(sizes, total_rows, span)
    copies = sum(group - 1 for _, group, _, _ in plan)
    return pl.pallas_call(
        functools.partial(reduce_kernel, sizes, plan),
        out_shape=jax.ShapeDtypeStruct((rows, LANES), jnp.float32),
        in_specs=[VMEM],
        out_specs=VMEM,
        scratch_shapes=[
            pltpu.VMEM((group - 1, after, LANES), jnp.float32) for _, group, _, after in plan
        ]
        + [pltpu.VMEM((after, LANES), jnp.float32) for _, _, _, after in plan[:-1]]
        + [pltpu.SemaphoreType.DMA((copies,)), pltpu.SemaphoreType.DMA((copies,))],
        compiler_params=pltpu.CompilerParams(
            collective_id=1, has_side_effects=True, vmem_limit_bytes=VMEM_LIMIT
        ),
    )(partial)


def solve_kernel(total_range, gram_ref, right_ref, out_ref):
    span = right_ref.shape[1]
    pairs = gram_ref.shape[0] // span
    rows = lax.broadcasted_iota(jnp.int32, (span, LANES), 0)
    lanes = lax.broadcasted_iota(jnp.int32, (span, LANES), 1)
    scale = 1.0 / total_range
    systems = []
    for pair in range(pairs):
        packed = gram_ref[pair * span : (pair + 1) * span, :] * scale
        padded = jnp.concatenate(
            [packed, jnp.zeros((LANES - span, LANES), jnp.float32)], axis=0
        )
        turned = padded.T
        for s in range(2):
            here = packed if s == 0 else pltpu.roll(packed, LANES - span, axis=1)
            there = turned[s * span : (s + 1) * span, :]
            real = jnp.where(rows <= lanes, here, there)
            imag = jnp.where(rows > lanes, here, jnp.where(rows < lanes, -there, 0.0))
            b = 2 * pair + s
            real = jnp.where(lanes < span, real, jnp.where(lanes == span, right_ref[2 * b], 0.0))
            imag = jnp.where(
                lanes < span, imag, jnp.where(lanes == span, right_ref[2 * b + 1], 0.0)
            )
            systems.append((real, imag))
    for k in range(span):
        for b, (real, imag) in enumerate(systems):
            inverse = 1.0 / real[k : k + 1, k : k + 1]
            row_real = real[k : k + 1, :] * inverse
            row_imag = imag[k : k + 1, :] * inverse
            col_real = real[:, k : k + 1]
            col_imag = imag[:, k : k + 1]
            pivot = rows == k
            next_real = jnp.where(
                pivot, row_real, real - (col_real * row_real - col_imag * row_imag)
            )
            next_imag = jnp.where(
                pivot, row_imag, imag - (col_real * row_imag + col_imag * row_real)
            )
            systems[b] = (next_real, next_imag)
    columns = jnp.zeros((span, LANES), jnp.float32)
    for b, (real, imag) in enumerate(systems):
        columns = jnp.where(lanes == 2 * b, real[:, span : span + 1], columns)
        columns = jnp.where(lanes == 2 * b + 1, imag[:, span : span + 1], columns)
    padded = jnp.concatenate([columns, jnp.zeros((LANES - span, LANES), jnp.float32)], axis=0)
    out_ref[...] = padded.T[: out_ref.shape[0], :]


def solve(own_gram, right, total_range):
    held = -(-right.shape[0] // 8) * 8
    return pl.pallas_call(
        functools.partial(solve_kernel, total_range),
        out_shape=jax.ShapeDtypeStruct((held, LANES), jnp.float32),
        in_specs=[VMEM, VMEM],
        out_specs=VMEM,
    )(own_gram, right)


def weights_kernel(sizes, own_ref, out_ref, send_sems, recv_sems, local_sem):
    count = out_ref.shape[0]
    me = chunk_index(sizes, my_parts(sizes))
    devices = [place_of(sizes, (me + k) % count) for k in range(1, count)]
    greet(devices)
    copies = []
    for k, device in enumerate(devices):
        copies.append(
            pltpu.make_async_remote_copy(
                src_ref=own_ref,
                dst_ref=out_ref.at[me],
                send_sem=send_sems.at[k],
                recv_sem=recv_sems.at[k],
                device_id=device,
                device_id_type=MESH,
            )
        )
        copies[-1].start()
    own = pltpu.make_async_copy(own_ref, out_ref.at[me], local_sem)
    own.start()
    own.wait()
    for copy in copies:
        copy.wait()


def gather_weights(own, sizes):
    count = sizes[0] * sizes[1] * sizes[2] * sizes[3]
    return pl.pallas_call(
        functools.partial(weights_kernel, sizes),
        out_shape=jax.ShapeDtypeStruct((count,) + own.shape, jnp.float32),
        in_specs=[VMEM],
        out_specs=VMEM,
        scratch_shapes=[
            pltpu.SemaphoreType.DMA((count - 1,)),
            pltpu.SemaphoreType.DMA((count - 1,)),
            pltpu.SemaphoreType.DMA,
        ],
        compiler_params=pltpu.CompilerParams(collective_id=2, has_side_effects=True),
    )(own)


def power_kernel(owned, trip_ref, echo_ref, weight_ref, out_ref, turned_ref):
    slots = trip_ref.shape[1]
    held = weight_ref.shape[1]
    span = turned_ref.shape[1]
    owners = trip_ref.shape[0] // owned
    per_tile = LANES // held
    for tile in range(turned_ref.shape[0]):
        block = weight_ref[tile * per_tile : (tile + 1) * per_tile].reshape(LANES, LANES)
        turned_ref[tile] = block.T[:span, :]

    def owner_step(owner, carry):
        shift = (owner % per_tile) * held
        rolled = pltpu.roll(turned_ref[owner // per_tile], (LANES - shift) % LANES, axis=1)
        for k in range(owned):
            b = owner * owned + k
            wr = rolled[:, 2 * k : 2 * k + 1]
            wi = rolled[:, 2 * k + 1 : 2 * k + 2]
            u = jnp.concatenate([echo_ref[0, trip_ref[b, t]] for t in range(slots)], axis=0)
            v = jnp.concatenate([echo_ref[1, trip_ref[b, t]] for t in range(slots)], axis=0)
            yr = jnp.sum(wr * u + wi * v, axis=0, keepdims=True)
            yi = jnp.sum(wr * v - wi * u, axis=0, keepdims=True)
            out_ref[pl.ds(b, 1), :] = yr * yr + yi * yi
        return carry

    lax.fori_loop(0, owners, owner_step, 0)


def apply_weights(triplet, echoes, weights, owned):
    bins, slots = triplet.shape
    chans, gates = echoes.shape[2:]
    tiles = (bins // owned) * weights.shape[1] // LANES
    return pl.pallas_call(
        functools.partial(power_kernel, owned),
        out_shape=jax.ShapeDtypeStruct((bins, gates), jnp.float32),
        in_specs=[SMEM, VMEM, VMEM],
        out_specs=VMEM,
        scratch_shapes=[pltpu.VMEM((tiles, slots * chans, LANES), jnp.float32)],
        compiler_params=pltpu.CompilerParams(vmem_limit_bytes=VMEM_LIMIT),
    )(triplet, echoes, weights)


def exchange_kernel(sizes, power_ref, out_ref, send_sems, recv_sems, local_sem):
    dops = sizes[1]
    ranges = sizes[0] * sizes[2] * sizes[3]
    bins = out_ref.shape[0]
    gates = power_ref.shape[1]
    r = lax.axis_index("range")
    y = lax.axis_index("dop")
    last = ranges - 1
    left_row = (r + last) % ranges
    right_row = (r + 1) % ranges
    greet(
        [(r, (y + k) % dops) for k in range(1, dops)]
        + [(left_row, k) for k in range(dops)]
        + [(right_row, k) for k in range(dops)]
    )
    middle = LANES + pl.multiple_of(y * gates, LANES)
    copies = []
    for k in range(1, dops):
        target = (y + k) % dops
        copies.append(
            pltpu.make_async_remote_copy(
                src_ref=power_ref.at[pl.ds(pl.multiple_of(target * bins, 8), bins), :],
                dst_ref=out_ref.at[:, pl.ds(middle, gates)],
                send_sem=send_sems.at[k - 1],
                recv_sem=recv_sems.at[k - 1],
                device_id=(r, target),
                device_id_type=MESH,
            )
        )
        copies[-1].start()

    def halo(k, to_right):
        source = gates - LANES if to_right else 0
        target = LANES + dops * gates if not to_right else 0
        number = dops - 1 + k + (dops if to_right else 0)
        return pltpu.make_async_remote_copy(
            src_ref=power_ref.at[k * bins : (k + 1) * bins, source : source + LANES],
            dst_ref=out_ref.at[:, target : target + LANES],
            send_sem=send_sems.at[number],
            recv_sem=recv_sems.at[dops - 1 + (1 if to_right else 0)],
            device_id=(right_row if to_right else left_row, k),
            device_id_type=MESH,
        )

    sends_right = jnp.logical_and(y == dops - 1, r < last)
    sends_left = jnp.logical_and(y == 0, r > 0)

    @pl.when(sends_right)
    def _():
        for k in range(dops):
            halo(k, True).start()

    @pl.when(sends_left)
    def _():
        for k in range(dops):
            halo(k, False).start()

    own = pltpu.make_async_copy(
        power_ref.at[pl.ds(pl.multiple_of(y * bins, 8), bins), :],
        out_ref.at[:, pl.ds(middle, gates)],
        local_sem,
    )
    own.start()

    @pl.when(r == 0)
    def _():
        out_ref[:, :LANES] = jnp.zeros((bins, LANES), jnp.float32)

    @pl.when(r == last)
    def _():
        out_ref[:, LANES + dops * gates :] = jnp.zeros((bins, LANES), jnp.float32)

    own.wait()
    for copy in copies:
        copy.wait()

    @pl.when(sends_right)
    def _():
        for k in range(dops):
            halo(k, True).wait_send()

    @pl.when(sends_left)
    def _():
        for k in range(dops):
            halo(k, False).wait_send()

    @pl.when(r > 0)
    def _():
        halo(0, True).wait_recv()

    @pl.when(r < last)
    def _():
        halo(0, False).wait_recv()


def exchange_power(power, sizes):
    bins, gates = power.shape
    dops = sizes[1]
    return pl.pallas_call(
        functools.partial(exchange_kernel, sizes),
        out_shape=jax.ShapeDtypeStruct((bins // dops, dops * gates + 2 * LANES), jnp.float32),
        in_specs=[VMEM],
        out_specs=VMEM,
        scratch_shapes=[
            pltpu.SemaphoreType.DMA((3 * dops - 1,)),
            pltpu.SemaphoreType.DMA((dops + 1,)),
            pltpu.SemaphoreType.DMA,
        ],
        compiler_params=pltpu.CompilerParams(collective_id=3, has_side_effects=True),
    )(power)


def detect_kernel(total_range, padded_ref, guard_ref, train_ref, out_ref):
    width = padded_ref.shape[1]
    cells = out_ref.shape[1]
    padded = padded_ref[...]
    guard = guard_ref[...]
    train = train_ref[...]

    def ahead(values, by):
        return pltpu.roll(values, (width - by) % width, axis=1)

    def behind(values, by):
        return pltpu.roll(values, by % width, axis=1)

    forward = padded
    right = jnp.zeros_like(padded)
    left = jnp.zeros_like(padded)
    step = 1
    while step <= TRAIN_MAX:
        chosen = (train & step) != 0
        backward = behind(forward, step - 1) if step > 1 else forward
        right = jnp.where(chosen, forward + ahead(right, step), right)
        left = jnp.where(chosen, backward + behind(left, step), left)
        forward = forward + ahead(forward, step)
        step *= 2
    total = jnp.zeros_like(padded)
    for size in range(1, GUARD_MAX + 1):
        both = ahead(right, size + 1) + behind(left, size + 1)
        total = jnp.where(guard == size, both, total)
    start = lax.axis_index("range") * cells
    position = start + lax.broadcasted_iota(jnp.int32, (out_ref.shape[0], cells), 1)
    left_count = jnp.maximum(
        jnp.minimum(position - guard - 1, total_range - 1)
        - jnp.maximum(position - guard - train, 0)
        + 1,
        0,
    )
    right_count = jnp.maximum(
        jnp.minimum(position + guard + train, total_range - 1)
        - jnp.maximum(position + guard + 1, 0)
        + 1,
        0,
    )
    noise = total[:, LANES : LANES + cells] / (left_count + right_count).astype(jnp.float32)
    out_ref[...] = padded[:, LANES : LANES + cells] / (noise + epsilon)


def detect(padded, guard_len, train_len, total_range):
    bins, width = padded.shape
    return pl.pallas_call(
        functools.partial(detect_kernel, total_range),
        out_shape=jax.ShapeDtypeStruct((bins, width - 2 * LANES), jnp.float32),
        in_specs=[VMEM, VMEM, VMEM],
        out_specs=VMEM,
    )(padded, guard_len[:, None], train_len[:, None])


def shards(echoes, triplet, bin_taper, phases, excluded, guard_len, train_len):
    bins, slots = triplet.shape
    chans = echoes.shape[2]
    span = slots * chans
    ranges = lax.axis_size("range")
    dops = lax.axis_size("dop")
    sizes = grid_sizes(ranges, dops)
    total_range = excluded.shape[1] * BLOCK * ranges
    partial = gram(triplet, echoes, gather_mask(excluded, dops))
    own_gram = reduce_grams(partial.reshape(bins // 2 * span, LANES), sizes, span)
    owned = own_gram.shape[0] // span * 2
    owner = chunk_index(sizes, my_parts(sizes)) % (bins // owned)
    taper = lax.dynamic_slice_in_dim(bin_taper, owner * owned, owned, 0)
    turns = jnp.stack([jnp.cos(phases), jnp.sin(phases)])
    right = (taper[:, None, :, None] * turns[None, :, None, :]).reshape(2 * owned, span, 1)
    own_weights = solve(own_gram, right, total_range)
    weights = gather_weights(own_weights, sizes)
    power = apply_weights(triplet, echoes, weights, owned)
    padded = exchange_power(power, sizes)
    return detect(padded, guard_len, train_len, total_range)


def solution(mesh):
    placed = (
        P(None, None, None, ("range", "dop")),
        P(),
        P(),
        P(),
        P("dop", "range"),
        P("dop"),
        P("dop"),
    )
    return jax.shard_map(
        shards, mesh=mesh, in_specs=placed, out_specs=P("dop", "range"), check_vma=False
    )
```

```python
import functools

import jax
import jax.numpy as jnp
from jax import lax
from jax.experimental import pallas as pl
from jax.experimental.pallas import tpu as pltpu
from jax.sharding import PartitionSpec as P

BLOCK = 16
GUARD_MAX = 4
TRAIN_MAX = 64
LANES = 128
epsilon = 1e-06

MESH = pl.DeviceIdType.MESH
VMEM = pl.BlockSpec(memory_space=pltpu.VMEM)
SMEM = pl.BlockSpec(memory_space=pltpu.SMEM)
VMEM_LIMIT = 60 * 1024 * 1024


def grid_sizes(range_count, dop_count):
    core = 2 if range_count % 2 == 0 else 1
    rest = range_count // core
    near = 1
    while near * near * 4 <= rest and rest % (near * 2) == 0:
        near *= 2
    return core, dop_count, near, rest // near


def place_of(sizes, index):
    core, dops, near, far = sizes
    c = index // (dops * near * far)
    y = (index // (near * far)) % dops
    x = (index // far) % near
    z = index % far
    return ((z * near + x) * core + c, y)


def my_parts(sizes):
    core, _, near, _ = sizes
    r = lax.axis_index("range")
    return r % core, lax.axis_index("dop"), (r // core) % near, r // (core * near)


def chunk_index(sizes, parts):
    core, dops, near, far = sizes
    c, y, x, z = parts
    return ((c * dops + y) * near + x) * far + z


def greet(devices):
    barrier = pltpu.get_barrier_semaphore()
    for device in devices:
        pl.semaphore_signal(barrier, inc=1, device_id=device, device_id_type=MESH)
    pl.semaphore_wait(barrier, len(devices))


def stream_plan(sizes, pairs):
    count = sizes[0] * sizes[1] * sizes[2] * sizes[3]
    split_core = pairs % count == 0 and sizes[0] == 2
    streams = pairs // count if split_core else pairs // (count // sizes[0])
    return split_core, streams


def gram_kernel(sizes, trip_ref, echo_ref, excl_ref, out_ref, *scratch):
    (mask_ref, kept_ref, other_ref, from_core, own_ref, total_ref, recv_first, mid_ref,
     recv_second, low_ref, recv_third, mask_send, mask_recv, send_sems, recv_sems) = scratch
    core, dops, near, far = sizes
    slots = trip_ref.shape[1]
    chans, gates = echo_ref.shape[2:]
    span = slots * chans
    blocks = excl_ref.shape[1]
    split_core, streams = stream_plan(sizes, trip_ref.shape[0] // 2)
    swap = 1 if streams > 1 and dops == near else 0
    half = dops * near * far
    block = half // dops
    parts = my_parts(sizes)
    c, y, x, z = parts

    def device(axis, k):
        moved = list(parts)
        moved[axis] = (parts[axis] + k) % sizes[axis]
        return place_of(sizes, chunk_index(sizes, moved))

    greet([device(axis, k) for axis in range(4) for k in range(1, sizes[axis])])

    def send(source, target, axis, k, sem, sends=send_sems, recvs=recv_sems):
        copy = pltpu.make_async_remote_copy(
            src_ref=source,
            dst_ref=target,
            send_sem=sends.at[sem],
            recv_sem=recvs.at[sem],
            device_id=device(axis, k),
            device_id_type=MESH,
        )
        copy.start()
        return copy

    masks = [
        send(excl_ref, mask_ref.at[y], 1, k, k - 1, mask_send, mask_recv)
        for k in range(1, dops)
    ]
    mask_ref[y] = excl_ref[...]
    block_ids = lax.broadcasted_iota(jnp.int32, (blocks, gates), 0)
    gate_blocks = lax.broadcasted_iota(jnp.int32, (blocks, gates), 1) // BLOCK
    spread = jnp.where(
        block_ids == gate_blocks + y * (gates // BLOCK), 1.0, 0.0
    ).astype(jnp.bfloat16)
    for copy in masks:
        copy.wait()
    for d in range(dops):
        rows_here = excl_ref.shape[0]
        kept_ref[d * rows_here : (d + 1) * rows_here, :] = 1.0 - jnp.dot(
            mask_ref[d].astype(jnp.float32).astype(jnp.bfloat16),
            spread,
            preferred_element_type=jnp.float32,
        )
    rows = lax.broadcasted_iota(jnp.int32, (span, LANES), 0)
    lanes = lax.broadcasted_iota(jnp.int32, (span, LANES), 1)
    upper_even = rows <= lanes
    upper_odd = rows <= lanes - span
    is_even = lanes < span
    filler = jnp.zeros((LANES - 2 * span, 8 * gates), jnp.bfloat16)

    def split(values):
        high = values.astype(jnp.bfloat16)
        return high, (values - high.astype(jnp.float32)).astype(jnp.bfloat16)

    def pair_gram(which, s, pos):
        q = pos // block
        second = (pos // far) % near
        turn = s * swap
        at_y = q + turn * (second - q)
        at_x = second + turn * (q - second)
        owner = (which * dops + at_y) * near + at_x
        pair = streams * (owner * far + pos % far) + s
        lefts = []
        rights = []
        for e in range(2):
            b = 2 * pair + e
            u = jnp.concatenate([echo_ref[0, trip_ref[b, t]] for t in range(slots)], axis=0)
            v = jnp.concatenate([echo_ref[1, trip_ref[b, t]] for t in range(slots)], axis=0)
            kept = kept_ref[pl.ds(b, 1), :].astype(jnp.bfloat16)
            uh, ul = split(u)
            vh, vl = split(v)
            uhm, ulm, vhm, vlm = uh * kept, ul * kept, vh * kept, vl * kept
            rights.append(jnp.concatenate([uh, vh, uh, vh, ul, vl, ul, vl], axis=1))
            lefts.append(jnp.concatenate([uhm, vhm, ulm, vlm] * 2, axis=1))
            lefts.append(jnp.concatenate([vhm, -uhm, vlm, -ulm] * 2, axis=1))
        left = jnp.concatenate(lefts, axis=0)
        right = jnp.concatenate(rights + [filler], axis=0)
        product = lax.dot_general(
            left, right, (((1,), (1,)), ((), ())), preferred_element_type=jnp.float32
        )
        even = jnp.where(upper_even, product[:span], product[span : 2 * span])
        odd = jnp.where(upper_odd, product[2 * span : 3 * span], product[3 * span :])
        return jnp.where(is_even, even, odd)

    which = c if split_core else 0
    mine = [x if s * swap else y for s in range(streams)]
    mine_first = mine[0]
    mine_rest = mine[-1] if streams > 1 else mine[0]

    def own_loop(first, count):
        def step(i, carry):
            s = i // (count * block)
            j = i % (count * block)
            me = mine_first + jnp.minimum(s, 1) * (mine_rest - mine_first)
            pos = ((me + first + j // block) % dops) * block + j % block
            own_ref[s * half + pos] = pair_gram(which, s, pos)
            return carry

        lax.fori_loop(0, streams * count * block, step, 0)

    sem = 0
    core_copy = None
    if split_core:

        def other_step(i, carry):
            other_ref[i] = pair_gram((c + 1) % core, i // half, i % half)
            return carry

        lax.fori_loop(0, streams * half, other_step, 0)
        core_copy = send(other_ref, from_core, 0, 1, sem)
        sem += 1
        own_loop(1, dops - 1)
    else:
        own_loop(1, dops)
        if core == 2:
            core_copy = send(own_ref, from_core, 0, 1, sem)
            sem += 1
    if core_copy is not None:
        core_copy.wait()

    def summed(s, q):
        place = pl.ds(s * half + q * block, block)
        value = own_ref[place]
        return value + from_core[place] if core_copy is not None else value

    copies = [[] for _ in range(streams)]
    for s in range(streams):
        for k in range(1, dops):
            q = (mine[s] + k) % dops
            total_ref[s, k - 1] = summed(s, q)
            copies[s].append(
                send(
                    total_ref.at[s, k - 1],
                    recv_first.at[s, k - 1],
                    2 if s * swap else 1,
                    k,
                    sem,
                )
            )
            sem += 1
    if split_core:
        own_loop(0, 1)
    second_copies = [[] for _ in range(streams)]
    for s in range(streams):
        value = summed(s, mine[s])
        for k in range(1, dops):
            copies[s][k - 1].wait()
            value = value + recv_first[s, k - 1]
        mid_ref[s] = value
        axis = 1 if s * swap else 2
        for k in range(1, near):
            q = (parts[axis] + k) % near
            second_copies[s].append(
                send(
                    mid_ref.at[s, pl.ds(q * far, far)], recv_second.at[s, k - 1], axis, k, sem
                )
            )
            sem += 1
    third_copies = [[] for _ in range(streams)]
    for s in range(streams):
        axis = 1 if s * swap else 2
        value = mid_ref[s, pl.ds(parts[axis] * far, far)]
        for k in range(1, near):
            second_copies[s][k - 1].wait()
            value = value + recv_second[s, k - 1]
        low_ref[s] = value
        for k in range(1, far):
            q = (z + k) % far
            third_copies[s].append(
                send(low_ref.at[s, q], recv_third.at[s, k - 1], 3, k, sem)
            )
            sem += 1
    for s in range(streams):
        value = low_ref[s, z]
        for k in range(1, far):
            third_copies[s][k - 1].wait()
            value = value + recv_third[s, k - 1]
        out_ref[s * span : (s + 1) * span, :] = value


def reduced_grams(triplet, echoes, excluded, sizes):
    bins, slots = triplet.shape
    chans, gates = echoes.shape[2:]
    span = slots * chans
    core, dops, near, far = sizes
    split_core, streams = stream_plan(sizes, bins // 2)
    half = dops * near * far
    block = half // dops
    sends = (core - 1) + streams * ((dops - 1) + (near - 1) + (far - 1))

    def buffer(*lead):
        return pltpu.VMEM(tuple(max(n, 1) for n in lead) + (span, LANES), jnp.float32)

    return pl.pallas_call(
        functools.partial(gram_kernel, sizes),
        out_shape=jax.ShapeDtypeStruct((streams * span, LANES), jnp.float32),
        in_specs=[SMEM, VMEM, VMEM],
        out_specs=VMEM,
        scratch_shapes=[
            pltpu.VMEM((dops,) + excluded.shape, jnp.int32),
            pltpu.VMEM((bins, gates), jnp.float32),
            buffer(streams * half if split_core else 1),
            buffer(streams * half),
            buffer(streams * half),
            buffer(streams, dops - 1, block),
            buffer(streams, dops - 1, block),
            buffer(streams, block),
            buffer(streams, near - 1, far),
            buffer(streams, far),
            buffer(streams, far - 1),
            pltpu.SemaphoreType.DMA((max(dops - 1, 1),)),
            pltpu.SemaphoreType.DMA((max(dops - 1, 1),)),
            pltpu.SemaphoreType.DMA((max(sends, 1),)),
            pltpu.SemaphoreType.DMA((max(sends, 1),)),
        ],
        compiler_params=pltpu.CompilerParams(
            collective_id=1, has_side_effects=True, vmem_limit_bytes=VMEM_LIMIT
        ),
    )(triplet, echoes, excluded)


def solve_kernel(total_range, gram_ref, right_ref, out_ref):
    span = right_ref.shape[1]
    pairs = gram_ref.shape[0] // span
    rows = lax.broadcasted_iota(jnp.int32, (span, LANES), 0)
    lanes = lax.broadcasted_iota(jnp.int32, (span, LANES), 1)
    scale = 1.0 / total_range
    systems = []
    for pair in range(pairs):
        packed = gram_ref[pair * span : (pair + 1) * span, :] * scale
        padded = jnp.concatenate(
            [packed, jnp.zeros((LANES - span, LANES), jnp.float32)], axis=0
        )
        turned = padded.T
        for s in range(2):
            here = packed if s == 0 else pltpu.roll(packed, LANES - span, axis=1)
            there = turned[s * span : (s + 1) * span, :]
            real = jnp.where(rows <= lanes, here, there)
            imag = jnp.where(rows > lanes, here, jnp.where(rows < lanes, -there, 0.0))
            b = 2 * pair + s
            real = jnp.where(lanes < span, real, jnp.where(lanes == span, right_ref[2 * b], 0.0))
            imag = jnp.where(
                lanes < span, imag, jnp.where(lanes == span, right_ref[2 * b + 1], 0.0)
            )
            systems.append((real, imag))
    for k in range(span):
        for b, (real, imag) in enumerate(systems):
            inverse = 1.0 / real[k : k + 1, k : k + 1]
            row_real = real[k : k + 1, :] * inverse
            row_imag = imag[k : k + 1, :] * inverse
            col_real = real[:, k : k + 1]
            col_imag = imag[:, k : k + 1]
            pivot = rows == k
            next_real = jnp.where(
                pivot, row_real, real - (col_real * row_real - col_imag * row_imag)
            )
            next_imag = jnp.where(
                pivot, row_imag, imag - (col_real * row_imag + col_imag * row_real)
            )
            systems[b] = (next_real, next_imag)
    columns = jnp.zeros((span, LANES), jnp.float32)
    for b, (real, imag) in enumerate(systems):
        columns = jnp.where(lanes == 2 * b, real[:, span : span + 1], columns)
        columns = jnp.where(lanes == 2 * b + 1, imag[:, span : span + 1], columns)
    padded = jnp.concatenate([columns, jnp.zeros((LANES - span, LANES), jnp.float32)], axis=0)
    out_ref[...] = padded.T[: out_ref.shape[0], :]


def solve(own_gram, right, total_range):
    held = -(-right.shape[0] // 8) * 8
    return pl.pallas_call(
        functools.partial(solve_kernel, total_range),
        out_shape=jax.ShapeDtypeStruct((held, LANES), jnp.float32),
        in_specs=[VMEM, VMEM],
        out_specs=VMEM,
    )(own_gram, right)


def weights_kernel(sizes, own_ref, out_ref, send_sems, recv_sems, local_sem):
    count = out_ref.shape[0]
    me = chunk_index(sizes, my_parts(sizes))
    devices = [place_of(sizes, (me + k) % count) for k in range(1, count)]
    greet(devices)
    copies = []
    for k, device in enumerate(devices):
        copies.append(
            pltpu.make_async_remote_copy(
                src_ref=own_ref,
                dst_ref=out_ref.at[me],
                send_sem=send_sems.at[k],
                recv_sem=recv_sems.at[k],
                device_id=device,
                device_id_type=MESH,
            )
        )
        copies[-1].start()
    own = pltpu.make_async_copy(own_ref, out_ref.at[me], local_sem)
    own.start()
    own.wait()
    for copy in copies:
        copy.wait()


def gather_weights(own, sizes):
    count = sizes[0] * sizes[1] * sizes[2] * sizes[3]
    return pl.pallas_call(
        functools.partial(weights_kernel, sizes),
        out_shape=jax.ShapeDtypeStruct((count,) + own.shape, jnp.float32),
        in_specs=[VMEM],
        out_specs=VMEM,
        scratch_shapes=[
            pltpu.SemaphoreType.DMA((count - 1,)),
            pltpu.SemaphoreType.DMA((count - 1,)),
            pltpu.SemaphoreType.DMA,
        ],
        compiler_params=pltpu.CompilerParams(collective_id=2, has_side_effects=True),
    )(own)


def power_kernel(owned, trip_ref, echo_ref, weight_ref, out_ref, turned_ref):
    slots = trip_ref.shape[1]
    held = weight_ref.shape[1]
    span = turned_ref.shape[1]
    owners = trip_ref.shape[0] // owned
    per_tile = LANES // held
    for tile in range(turned_ref.shape[0]):
        block = weight_ref[tile * per_tile : (tile + 1) * per_tile].reshape(LANES, LANES)
        turned_ref[tile] = block.T[:span, :]

    def owner_step(owner, carry):
        shift = (owner % per_tile) * held
        rolled = pltpu.roll(turned_ref[owner // per_tile], (LANES - shift) % LANES, axis=1)
        for k in range(owned):
            b = owner * owned + k
            wr = rolled[:, 2 * k : 2 * k + 1]
            wi = rolled[:, 2 * k + 1 : 2 * k + 2]
            u = jnp.concatenate([echo_ref[0, trip_ref[b, t]] for t in range(slots)], axis=0)
            v = jnp.concatenate([echo_ref[1, trip_ref[b, t]] for t in range(slots)], axis=0)
            yr = jnp.sum(wr * u + wi * v, axis=0, keepdims=True)
            yi = jnp.sum(wr * v - wi * u, axis=0, keepdims=True)
            out_ref[pl.ds(b, 1), :] = yr * yr + yi * yi
        return carry

    lax.fori_loop(0, owners, owner_step, 0, unroll=4)


def apply_weights(triplet, echoes, weights, owned):
    bins, slots = triplet.shape
    chans, gates = echoes.shape[2:]
    tiles = (bins // owned) * weights.shape[1] // LANES
    return pl.pallas_call(
        functools.partial(power_kernel, owned),
        out_shape=jax.ShapeDtypeStruct((bins, gates), jnp.float32),
        in_specs=[SMEM, VMEM, VMEM],
        out_specs=VMEM,
        scratch_shapes=[pltpu.VMEM((tiles, slots * chans, LANES), jnp.float32)],
        compiler_params=pltpu.CompilerParams(vmem_limit_bytes=VMEM_LIMIT),
    )(triplet, echoes, weights)


def exchange_kernel(sizes, power_ref, out_ref, send_sems, recv_sems, local_sem):
    dops = sizes[1]
    ranges = sizes[0] * sizes[2] * sizes[3]
    bins = out_ref.shape[0]
    gates = power_ref.shape[1]
    r = lax.axis_index("range")
    y = lax.axis_index("dop")
    last = ranges - 1
    left_row = (r + last) % ranges
    right_row = (r + 1) % ranges
    greet(
        [(r, (y + k) % dops) for k in range(1, dops)]
        + [(left_row, k) for k in range(dops)]
        + [(right_row, k) for k in range(dops)]
    )
    middle = LANES + pl.multiple_of(y * gates, LANES)
    copies = []
    for k in range(1, dops):
        target = (y + k) % dops
        copies.append(
            pltpu.make_async_remote_copy(
                src_ref=power_ref.at[pl.ds(pl.multiple_of(target * bins, 8), bins), :],
                dst_ref=out_ref.at[:, pl.ds(middle, gates)],
                send_sem=send_sems.at[k - 1],
                recv_sem=recv_sems.at[k - 1],
                device_id=(r, target),
                device_id_type=MESH,
            )
        )
        copies[-1].start()

    def halo(k, to_right):
        source = gates - LANES if to_right else 0
        target = LANES + dops * gates if not to_right else 0
        number = dops - 1 + k + (dops if to_right else 0)
        return pltpu.make_async_remote_copy(
            src_ref=power_ref.at[k * bins : (k + 1) * bins, source : source + LANES],
            dst_ref=out_ref.at[:, target : target + LANES],
            send_sem=send_sems.at[number],
            recv_sem=recv_sems.at[dops - 1 + (1 if to_right else 0)],
            device_id=(right_row if to_right else left_row, k),
            device_id_type=MESH,
        )

    sends_right = jnp.logical_and(y == dops - 1, r < last)
    sends_left = jnp.logical_and(y == 0, r > 0)

    @pl.when(sends_right)
    def _():
        for k in range(dops):
            halo(k, True).start()

    @pl.when(sends_left)
    def _():
        for k in range(dops):
            halo(k, False).start()

    own = pltpu.make_async_copy(
        power_ref.at[pl.ds(pl.multiple_of(y * bins, 8), bins), :],
        out_ref.at[:, pl.ds(middle, gates)],
        local_sem,
    )
    own.start()

    @pl.when(r == 0)
    def _():
        out_ref[:, :LANES] = jnp.zeros((bins, LANES), jnp.float32)

    @pl.when(r == last)
    def _():
        out_ref[:, LANES + dops * gates :] = jnp.zeros((bins, LANES), jnp.float32)

    own.wait()
    for copy in copies:
        copy.wait()

    @pl.when(sends_right)
    def _():
        for k in range(dops):
            halo(k, True).wait_send()

    @pl.when(sends_left)
    def _():
        for k in range(dops):
            halo(k, False).wait_send()

    @pl.when(r > 0)
    def _():
        halo(0, True).wait_recv()

    @pl.when(r < last)
    def _():
        halo(0, False).wait_recv()


def exchange_power(power, sizes):
    bins, gates = power.shape
    dops = sizes[1]
    return pl.pallas_call(
        functools.partial(exchange_kernel, sizes),
        out_shape=jax.ShapeDtypeStruct((bins // dops, dops * gates + 2 * LANES), jnp.float32),
        in_specs=[VMEM],
        out_specs=VMEM,
        scratch_shapes=[
            pltpu.SemaphoreType.DMA((3 * dops - 1,)),
            pltpu.SemaphoreType.DMA((dops + 1,)),
            pltpu.SemaphoreType.DMA,
        ],
        compiler_params=pltpu.CompilerParams(collective_id=3, has_side_effects=True),
    )(power)


def detect_kernel(total_range, padded_ref, guard_ref, train_ref, out_ref):
    width = padded_ref.shape[1]
    cells = out_ref.shape[1]
    padded = padded_ref[...]
    guard = guard_ref[...]
    train = train_ref[...]

    def ahead(values, by):
        return pltpu.roll(values, (width - by) % width, axis=1)

    def behind(values, by):
        return pltpu.roll(values, by % width, axis=1)

    forward = padded
    right = jnp.zeros_like(padded)
    left = jnp.zeros_like(padded)
    step = 1
    while step <= TRAIN_MAX:
        chosen = (train & step) != 0
        backward = behind(forward, step - 1) if step > 1 else forward
        right = jnp.where(chosen, forward + ahead(right, step), right)
        left = jnp.where(chosen, backward + behind(left, step), left)
        forward = forward + ahead(forward, step)
        step *= 2
    total = jnp.zeros_like(padded)
    for size in range(1, GUARD_MAX + 1):
        both = ahead(right, size + 1) + behind(left, size + 1)
        total = jnp.where(guard == size, both, total)
    start = lax.axis_index("range") * cells
    position = start + lax.broadcasted_iota(jnp.int32, (out_ref.shape[0], cells), 1)
    left_count = jnp.maximum(
        jnp.minimum(position - guard - 1, total_range - 1)
        - jnp.maximum(position - guard - train, 0)
        + 1,
        0,
    )
    right_count = jnp.maximum(
        jnp.minimum(position + guard + train, total_range - 1)
        - jnp.maximum(position + guard + 1, 0)
        + 1,
        0,
    )
    noise = total[:, LANES : LANES + cells] / (left_count + right_count).astype(jnp.float32)
    out_ref[...] = padded[:, LANES : LANES + cells] / (noise + epsilon)


def detect(padded, guard_len, train_len, total_range):
    bins, width = padded.shape
    return pl.pallas_call(
        functools.partial(detect_kernel, total_range),
        out_shape=jax.ShapeDtypeStruct((bins, width - 2 * LANES), jnp.float32),
        in_specs=[VMEM, VMEM, VMEM],
        out_specs=VMEM,
    )(padded, guard_len[:, None], train_len[:, None])


def shards(echoes, triplet, bin_taper, phases, excluded, guard_len, train_len):
    bins, slots = triplet.shape
    chans = echoes.shape[2]
    span = slots * chans
    ranges = lax.axis_size("range")
    dops = lax.axis_size("dop")
    sizes = grid_sizes(ranges, dops)
    total_range = excluded.shape[1] * BLOCK * ranges
    own_gram = reduced_grams(triplet, echoes, excluded, sizes)
    owned = own_gram.shape[0] // span * 2
    owner = chunk_index(sizes, my_parts(sizes)) % (bins // owned)
    taper = lax.dynamic_slice_in_dim(bin_taper, owner * owned, owned, 0)
    turns = jnp.stack([jnp.cos(phases), jnp.sin(phases)])
    right = (taper[:, None, :, None] * turns[None, :, None, :]).reshape(2 * owned, span, 1)
    own_weights = solve(own_gram, right, total_range)
    weights = gather_weights(own_weights, sizes)
    power = apply_weights(triplet, echoes, weights, owned)
    padded = exchange_power(power, sizes)
    return detect(padded, guard_len, train_len, total_range)


def solution(mesh):
    placed = (
        P(None, None, None, ("range", "dop")),
        P(),
        P(),
        P(),
        P("dop", "range"),
        P("dop"),
        P("dop"),
    )
    return jax.shard_map(
        shards, mesh=mesh, in_specs=placed, out_specs=P("dop", "range"), check_vma=False
    )
```

```python
import functools

import jax
import jax.numpy as jnp
from jax import lax
from jax.experimental import pallas as pl
from jax.experimental.pallas import tpu as pltpu
from jax.sharding import PartitionSpec as P

BLOCK = 16
GUARD_MAX = 4
TRAIN_MAX = 64
LANES = 128
epsilon = 1e-06

MESH = pl.DeviceIdType.MESH
VMEM = pl.BlockSpec(memory_space=pltpu.VMEM)
SMEM = pl.BlockSpec(memory_space=pltpu.SMEM)
VMEM_LIMIT = 60 * 1024 * 1024


def grid_sizes(range_count, dop_count):
    core = 2 if range_count % 2 == 0 else 1
    rest = range_count // core
    near = 1
    while near * near * 4 <= rest and rest % (near * 2) == 0:
        near *= 2
    return core, dop_count, near, rest // near


def place_of(sizes, index):
    core, dops, near, far = sizes
    c = index // (dops * near * far)
    y = (index // (near * far)) % dops
    x = (index // far) % near
    z = index % far
    return ((z * near + x) * core + c, y)


def my_parts(sizes):
    core, _, near, _ = sizes
    r = lax.axis_index("range")
    return r % core, lax.axis_index("dop"), (r // core) % near, r // (core * near)


def chunk_index(sizes, parts):
    core, dops, near, far = sizes
    c, y, x, z = parts
    return ((c * dops + y) * near + x) * far + z


def greet(devices):
    barrier = pltpu.get_barrier_semaphore()
    for device in devices:
        pl.semaphore_signal(barrier, inc=1, device_id=device, device_id_type=MESH)
    pl.semaphore_wait(barrier, len(devices))


def stream_plan(sizes, pairs):
    count = sizes[0] * sizes[1] * sizes[2] * sizes[3]
    split_core = pairs % count == 0 and sizes[0] == 2
    streams = pairs // count if split_core else pairs // (count // sizes[0])
    return split_core, streams


def gram_kernel(sizes, trip_ref, echo_ref, excl_ref, out_ref, *scratch):
    (mask_ref, kept_ref, other_ref, from_core, own_ref, total_ref, recv_first, mid_ref,
     recv_second, low_ref, recv_third, mask_send, mask_recv, send_sems, recv_sems) = scratch
    core, dops, near, far = sizes
    slots = trip_ref.shape[0]
    chans, gates = echo_ref.shape[2:]
    span = slots * chans
    blocks = excl_ref.shape[0]
    split_core, streams = stream_plan(sizes, trip_ref.shape[1] // 2)
    swap = 1 if streams > 1 and dops == near else 0
    half = dops * near * far
    block = half // dops
    parts = my_parts(sizes)
    c, y, x, z = parts

    def device(axis, k):
        moved = list(parts)
        moved[axis] = (parts[axis] + k) % sizes[axis]
        return place_of(sizes, chunk_index(sizes, moved))

    greet([device(axis, k) for axis in range(4) for k in range(1, sizes[axis])])

    def send(source, target, axis, k, sem, sends=send_sems, recvs=recv_sems):
        copy = pltpu.make_async_remote_copy(
            src_ref=source,
            dst_ref=target,
            send_sem=sends.at[sem],
            recv_sem=recvs.at[sem],
            device_id=device(axis, k),
            device_id_type=MESH,
        )
        copy.start()
        return copy

    masks = [
        send(excl_ref, mask_ref.at[y], 1, k, k - 1, mask_send, mask_recv)
        for k in range(1, dops)
    ]
    mask_ref[y] = excl_ref[...]
    block_ids = lax.broadcasted_iota(jnp.int32, (blocks, gates), 0)
    gate_blocks = lax.broadcasted_iota(jnp.int32, (blocks, gates), 1) // BLOCK
    spread = jnp.where(
        block_ids == gate_blocks + y * (gates // BLOCK), 1.0, 0.0
    ).astype(jnp.bfloat16)
    for copy in masks:
        copy.wait()
    for d in range(dops):
        rows_here = excl_ref.shape[1]
        kept_ref[d * rows_here : (d + 1) * rows_here, :] = 1.0 - lax.dot_general(
            mask_ref[d].astype(jnp.float32).astype(jnp.bfloat16),
            spread,
            (((0,), (0,)), ((), ())),
            preferred_element_type=jnp.float32,
        )
    rows = lax.broadcasted_iota(jnp.int32, (span, LANES), 0)
    lanes = lax.broadcasted_iota(jnp.int32, (span, LANES), 1)
    upper_even = rows <= lanes
    upper_odd = rows <= lanes - span
    is_even = lanes < span
    filler = jnp.zeros((LANES - 2 * span, 8 * gates), jnp.bfloat16)

    def split(values):
        high = values.astype(jnp.bfloat16)
        return high, (values - high.astype(jnp.float32)).astype(jnp.bfloat16)

    def pair_gram(which, s, pos):
        q = pos // block
        second = (pos // far) % near
        turn = s * swap
        at_y = q + turn * (second - q)
        at_x = second + turn * (q - second)
        owner = (which * dops + at_y) * near + at_x
        pair = streams * (owner * far + pos % far) + s
        lefts = []
        rights = []
        for e in range(2):
            b = 2 * pair + e
            u = jnp.concatenate([echo_ref[0, trip_ref[t, b]] for t in range(slots)], axis=0)
            v = jnp.concatenate([echo_ref[1, trip_ref[t, b]] for t in range(slots)], axis=0)
            kept = kept_ref[pl.ds(b, 1), :].astype(jnp.bfloat16)
            uh, ul = split(u)
            vh, vl = split(v)
            uhm, ulm, vhm, vlm = uh * kept, ul * kept, vh * kept, vl * kept
            rights.append(jnp.concatenate([uh, vh, uh, vh, ul, vl, ul, vl], axis=1))
            lefts.append(jnp.concatenate([uhm, vhm, ulm, vlm] * 2, axis=1))
            lefts.append(jnp.concatenate([vhm, -uhm, vlm, -ulm] * 2, axis=1))
        left = jnp.concatenate(lefts, axis=0)
        right = jnp.concatenate(rights + [filler], axis=0)
        product = lax.dot_general(
            left, right, (((1,), (1,)), ((), ())), preferred_element_type=jnp.float32
        )
        even = jnp.where(upper_even, product[:span], product[span : 2 * span])
        odd = jnp.where(upper_odd, product[2 * span : 3 * span], product[3 * span :])
        return jnp.where(is_even, even, odd)

    which = c if split_core else 0
    mine = [x if s * swap else y for s in range(streams)]
    mine_first = mine[0]
    mine_rest = mine[-1] if streams > 1 else mine[0]

    def own_loop(first, count):
        def step(i, carry):
            s = i // (count * block)
            j = i % (count * block)
            me = mine_first + jnp.minimum(s, 1) * (mine_rest - mine_first)
            pos = ((me + first + j // block) % dops) * block + j % block
            own_ref[s * half + pos] = pair_gram(which, s, pos)
            return carry

        lax.fori_loop(0, streams * count * block, step, 0, unroll=2)

    sem = 0
    core_copy = None
    if split_core:

        def other_step(i, carry):
            other_ref[i] = pair_gram((c + 1) % core, i // half, i % half)
            return carry

        lax.fori_loop(0, streams * half, other_step, 0, unroll=2)
        core_copy = send(other_ref, from_core, 0, 1, sem)
        sem += 1
        own_loop(1, dops - 1)
    else:
        own_loop(1, dops)
        if core == 2:
            core_copy = send(own_ref, from_core, 0, 1, sem)
            sem += 1
    if core_copy is not None:
        core_copy.wait()

    def summed(s, q):
        place = pl.ds(s * half + q * block, block)
        value = own_ref[place]
        return value + from_core[place] if core_copy is not None else value

    copies = [[] for _ in range(streams)]
    for s in range(streams):
        for k in range(1, dops):
            q = (mine[s] + k) % dops
            total_ref[s, k - 1] = summed(s, q)
            copies[s].append(
                send(
                    total_ref.at[s, k - 1],
                    recv_first.at[s, k - 1],
                    2 if s * swap else 1,
                    k,
                    sem,
                )
            )
            sem += 1
    if split_core:
        own_loop(0, 1)
    second_copies = [[] for _ in range(streams)]
    for s in range(streams):
        value = summed(s, mine[s])
        for k in range(1, dops):
            copies[s][k - 1].wait()
            value = value + recv_first[s, k - 1]
        mid_ref[s] = value
        axis = 1 if s * swap else 2
        for k in range(1, near):
            q = (parts[axis] + k) % near
            second_copies[s].append(
                send(
                    mid_ref.at[s, pl.ds(q * far, far)], recv_second.at[s, k - 1], axis, k, sem
                )
            )
            sem += 1
    third_copies = [[] for _ in range(streams)]
    for s in range(streams):
        axis = 1 if s * swap else 2
        value = mid_ref[s, pl.ds(parts[axis] * far, far)]
        for k in range(1, near):
            second_copies[s][k - 1].wait()
            value = value + recv_second[s, k - 1]
        low_ref[s] = value
        for k in range(1, far):
            q = (z + k) % far
            third_copies[s].append(
                send(low_ref.at[s, q], recv_third.at[s, k - 1], 3, k, sem)
            )
            sem += 1
    for s in range(streams):
        value = low_ref[s, z]
        for k in range(1, far):
            third_copies[s][k - 1].wait()
            value = value + recv_third[s, k - 1]
        out_ref[s * span : (s + 1) * span, :] = value


def reduced_grams(triplet, echoes, excluded, sizes):
    bins, slots = triplet.shape
    chans, gates = echoes.shape[2:]
    span = slots * chans
    core, dops, near, far = sizes
    split_core, streams = stream_plan(sizes, bins // 2)
    half = dops * near * far
    block = half // dops
    sends = (core - 1) + streams * ((dops - 1) + (near - 1) + (far - 1))

    def buffer(*lead):
        return pltpu.VMEM(tuple(max(n, 1) for n in lead) + (span, LANES), jnp.float32)

    return pl.pallas_call(
        functools.partial(gram_kernel, sizes),
        out_shape=jax.ShapeDtypeStruct((streams * span, LANES), jnp.float32),
        in_specs=[SMEM, VMEM, VMEM],
        out_specs=VMEM,
        scratch_shapes=[
            pltpu.VMEM((dops,) + excluded.T.shape, jnp.int32),
            pltpu.VMEM((bins, gates), jnp.float32),
            buffer(streams * half if split_core else 1),
            buffer(streams * half),
            buffer(streams * half),
            buffer(streams, dops - 1, block),
            buffer(streams, dops - 1, block),
            buffer(streams, block),
            buffer(streams, near - 1, far),
            buffer(streams, far),
            buffer(streams, far - 1),
            pltpu.SemaphoreType.DMA((max(dops - 1, 1),)),
            pltpu.SemaphoreType.DMA((max(dops - 1, 1),)),
            pltpu.SemaphoreType.DMA((max(sends, 1),)),
            pltpu.SemaphoreType.DMA((max(sends, 1),)),
        ],
        compiler_params=pltpu.CompilerParams(
            collective_id=1, has_side_effects=True, vmem_limit_bytes=VMEM_LIMIT
        ),
    )(triplet.T, echoes, excluded.T)


def solve_kernel(total_range, gram_ref, right_ref, out_ref):
    span = right_ref.shape[1]
    pairs = gram_ref.shape[0] // span
    rows = lax.broadcasted_iota(jnp.int32, (span, LANES), 0)
    lanes = lax.broadcasted_iota(jnp.int32, (span, LANES), 1)
    scale = 1.0 / total_range
    systems = []
    for pair in range(pairs):
        packed = gram_ref[pair * span : (pair + 1) * span, :] * scale
        padded = jnp.concatenate(
            [packed, jnp.zeros((LANES - span, LANES), jnp.float32)], axis=0
        )
        turned = padded.T
        for s in range(2):
            here = packed if s == 0 else pltpu.roll(packed, LANES - span, axis=1)
            there = turned[s * span : (s + 1) * span, :]
            real = jnp.where(rows <= lanes, here, there)
            imag = jnp.where(rows > lanes, here, jnp.where(rows < lanes, -there, 0.0))
            b = 2 * pair + s
            real = jnp.where(lanes < span, real, jnp.where(lanes == span, right_ref[2 * b], 0.0))
            imag = jnp.where(
                lanes < span, imag, jnp.where(lanes == span, right_ref[2 * b + 1], 0.0)
            )
            systems.append((real, imag))
    for k in range(span):
        for b, (real, imag) in enumerate(systems):
            inverse = 1.0 / real[k : k + 1, k : k + 1]
            row_real = real[k : k + 1, :] * inverse
            row_imag = imag[k : k + 1, :] * inverse
            col_real = real[:, k : k + 1]
            col_imag = imag[:, k : k + 1]
            pivot = rows == k
            next_real = jnp.where(
                pivot, row_real, real - (col_real * row_real - col_imag * row_imag)
            )
            next_imag = jnp.where(
                pivot, row_imag, imag - (col_real * row_imag + col_imag * row_real)
            )
            systems[b] = (next_real, next_imag)
    columns = jnp.zeros((span, LANES), jnp.float32)
    for b, (real, imag) in enumerate(systems):
        columns = jnp.where(lanes == 2 * b, real[:, span : span + 1], columns)
        columns = jnp.where(lanes == 2 * b + 1, imag[:, span : span + 1], columns)
    padded = jnp.concatenate([columns, jnp.zeros((LANES - span, LANES), jnp.float32)], axis=0)
    out_ref[...] = padded.T[: out_ref.shape[0], :]


def solve(own_gram, right, total_range):
    held = -(-right.shape[0] // 8) * 8
    return pl.pallas_call(
        functools.partial(solve_kernel, total_range),
        out_shape=jax.ShapeDtypeStruct((held, LANES), jnp.float32),
        in_specs=[VMEM, VMEM],
        out_specs=VMEM,
    )(own_gram, right)


def weights_kernel(sizes, own_ref, out_ref, send_sems, recv_sems, local_sem):
    count = out_ref.shape[0]
    me = chunk_index(sizes, my_parts(sizes))
    devices = [place_of(sizes, (me + k) % count) for k in range(1, count)]
    greet(devices)
    copies = []
    for k, device in enumerate(devices):
        copies.append(
            pltpu.make_async_remote_copy(
                src_ref=own_ref,
                dst_ref=out_ref.at[me],
                send_sem=send_sems.at[k],
                recv_sem=recv_sems.at[k],
                device_id=device,
                device_id_type=MESH,
            )
        )
        copies[-1].start()
    own = pltpu.make_async_copy(own_ref, out_ref.at[me], local_sem)
    own.start()
    own.wait()
    for copy in copies:
        copy.wait()


def gather_weights(own, sizes):
    count = sizes[0] * sizes[1] * sizes[2] * sizes[3]
    return pl.pallas_call(
        functools.partial(weights_kernel, sizes),
        out_shape=jax.ShapeDtypeStruct((count,) + own.shape, jnp.float32),
        in_specs=[VMEM],
        out_specs=VMEM,
        scratch_shapes=[
            pltpu.SemaphoreType.DMA((count - 1,)),
            pltpu.SemaphoreType.DMA((count - 1,)),
            pltpu.SemaphoreType.DMA,
        ],
        compiler_params=pltpu.CompilerParams(collective_id=2, has_side_effects=True),
    )(own)


def power_kernel(owned, trip_ref, echo_ref, weight_ref, out_ref, turned_ref):
    slots = trip_ref.shape[0]
    held = weight_ref.shape[1]
    span = turned_ref.shape[1]
    owners = trip_ref.shape[1] // owned
    per_tile = LANES // held
    for tile in range(turned_ref.shape[0]):
        block = weight_ref[tile * per_tile : (tile + 1) * per_tile].reshape(LANES, LANES)
        turned_ref[tile] = block.T[:span, :]

    def owner_step(owner, carry):
        shift = (owner % per_tile) * held
        rolled = pltpu.roll(turned_ref[owner // per_tile], (LANES - shift) % LANES, axis=1)
        for k in range(owned):
            b = owner * owned + k
            wr = rolled[:, 2 * k : 2 * k + 1]
            wi = rolled[:, 2 * k + 1 : 2 * k + 2]
            u = jnp.concatenate([echo_ref[0, trip_ref[t, b]] for t in range(slots)], axis=0)
            v = jnp.concatenate([echo_ref[1, trip_ref[t, b]] for t in range(slots)], axis=0)
            yr = jnp.sum(wr * u + wi * v, axis=0, keepdims=True)
            yi = jnp.sum(wr * v - wi * u, axis=0, keepdims=True)
            out_ref[pl.ds(b, 1), :] = yr * yr + yi * yi
        return carry

    lax.fori_loop(0, owners, owner_step, 0, unroll=4)


def apply_weights(triplet, echoes, weights, owned):
    bins, slots = triplet.shape
    chans, gates = echoes.shape[2:]
    tiles = (bins // owned) * weights.shape[1] // LANES
    return pl.pallas_call(
        functools.partial(power_kernel, owned),
        out_shape=jax.ShapeDtypeStruct((bins, gates), jnp.float32),
        in_specs=[SMEM, VMEM, VMEM],
        out_specs=VMEM,
        scratch_shapes=[pltpu.VMEM((tiles, slots * chans, LANES), jnp.float32)],
        compiler_params=pltpu.CompilerParams(vmem_limit_bytes=VMEM_LIMIT),
    )(triplet.T, echoes, weights)


def exchange_kernel(sizes, power_ref, out_ref, send_sems, recv_sems, local_sem):
    dops = sizes[1]
    ranges = sizes[0] * sizes[2] * sizes[3]
    bins = out_ref.shape[0]
    gates = power_ref.shape[1]
    r = lax.axis_index("range")
    y = lax.axis_index("dop")
    last = ranges - 1
    left_row = (r + last) % ranges
    right_row = (r + 1) % ranges
    greet(
        [(r, (y + k) % dops) for k in range(1, dops)]
        + [(left_row, k) for k in range(dops)]
        + [(right_row, k) for k in range(dops)]
    )
    middle = LANES + pl.multiple_of(y * gates, LANES)
    copies = []
    for k in range(1, dops):
        target = (y + k) % dops
        copies.append(
            pltpu.make_async_remote_copy(
                src_ref=power_ref.at[pl.ds(pl.multiple_of(target * bins, 8), bins), :],
                dst_ref=out_ref.at[:, pl.ds(middle, gates)],
                send_sem=send_sems.at[k - 1],
                recv_sem=recv_sems.at[k - 1],
                device_id=(r, target),
                device_id_type=MESH,
            )
        )
        copies[-1].start()

    def halo(k, to_right):
        source = gates - LANES if to_right else 0
        target = LANES + dops * gates if not to_right else 0
        number = dops - 1 + k + (dops if to_right else 0)
        return pltpu.make_async_remote_copy(
            src_ref=power_ref.at[k * bins : (k + 1) * bins, source : source + LANES],
            dst_ref=out_ref.at[:, target : target + LANES],
            send_sem=send_sems.at[number],
            recv_sem=recv_sems.at[dops - 1 + (1 if to_right else 0)],
            device_id=(right_row if to_right else left_row, k),
            device_id_type=MESH,
        )

    sends_right = jnp.logical_and(y == dops - 1, r < last)
    sends_left = jnp.logical_and(y == 0, r > 0)

    @pl.when(sends_right)
    def _():
        for k in range(dops):
            halo(k, True).start()

    @pl.when(sends_left)
    def _():
        for k in range(dops):
            halo(k, False).start()

    own = pltpu.make_async_copy(
        power_ref.at[pl.ds(pl.multiple_of(y * bins, 8), bins), :],
        out_ref.at[:, pl.ds(middle, gates)],
        local_sem,
    )
    own.start()

    @pl.when(r == 0)
    def _():
        out_ref[:, :LANES] = jnp.zeros((bins, LANES), jnp.float32)

    @pl.when(r == last)
    def _():
        out_ref[:, LANES + dops * gates :] = jnp.zeros((bins, LANES), jnp.float32)

    own.wait()
    for copy in copies:
        copy.wait()

    @pl.when(sends_right)
    def _():
        for k in range(dops):
            halo(k, True).wait_send()

    @pl.when(sends_left)
    def _():
        for k in range(dops):
            halo(k, False).wait_send()

    @pl.when(r > 0)
    def _():
        halo(0, True).wait_recv()

    @pl.when(r < last)
    def _():
        halo(0, False).wait_recv()


def exchange_power(power, sizes):
    bins, gates = power.shape
    dops = sizes[1]
    return pl.pallas_call(
        functools.partial(exchange_kernel, sizes),
        out_shape=jax.ShapeDtypeStruct((bins // dops, dops * gates + 2 * LANES), jnp.float32),
        in_specs=[VMEM],
        out_specs=VMEM,
        scratch_shapes=[
            pltpu.SemaphoreType.DMA((3 * dops - 1,)),
            pltpu.SemaphoreType.DMA((dops + 1,)),
            pltpu.SemaphoreType.DMA,
        ],
        compiler_params=pltpu.CompilerParams(collective_id=3, has_side_effects=True),
    )(power)


def detect_kernel(total_range, padded_ref, guard_ref, train_ref, out_ref):
    width = padded_ref.shape[1]
    cells = out_ref.shape[1]
    padded = padded_ref[...]

    def column(ref):
        row = jnp.broadcast_to(ref[...].astype(jnp.float32), (LANES, ref.shape[1]))
        return row.T[:, :1].astype(jnp.int32)

    guard = column(guard_ref)
    train = column(train_ref)

    def ahead(values, by):
        return pltpu.roll(values, (width - by) % width, axis=1)

    def behind(values, by):
        return pltpu.roll(values, by % width, axis=1)

    forward = padded
    right = jnp.zeros_like(padded)
    left = jnp.zeros_like(padded)
    step = 1
    while step <= TRAIN_MAX:
        chosen = (train & step) != 0
        backward = behind(forward, step - 1) if step > 1 else forward
        right = jnp.where(chosen, forward + ahead(right, step), right)
        left = jnp.where(chosen, backward + behind(left, step), left)
        forward = forward + ahead(forward, step)
        step *= 2
    total = jnp.zeros_like(padded)
    for size in range(1, GUARD_MAX + 1):
        both = ahead(right, size + 1) + behind(left, size + 1)
        total = jnp.where(guard == size, both, total)
    start = lax.axis_index("range") * cells
    position = start + lax.broadcasted_iota(jnp.int32, (out_ref.shape[0], cells), 1)
    left_count = jnp.maximum(
        jnp.minimum(position - guard - 1, total_range - 1)
        - jnp.maximum(position - guard - train, 0)
        + 1,
        0,
    )
    right_count = jnp.maximum(
        jnp.minimum(position + guard + train, total_range - 1)
        - jnp.maximum(position + guard + 1, 0)
        + 1,
        0,
    )
    noise = total[:, LANES : LANES + cells] / (left_count + right_count).astype(jnp.float32)
    out_ref[...] = padded[:, LANES : LANES + cells] / (noise + epsilon)


def detect(padded, guard_len, train_len, total_range):
    bins, width = padded.shape
    return pl.pallas_call(
        functools.partial(detect_kernel, total_range),
        out_shape=jax.ShapeDtypeStruct((bins, width - 2 * LANES), jnp.float32),
        in_specs=[VMEM, VMEM, VMEM],
        out_specs=VMEM,
    )(padded, guard_len[None, :], train_len[None, :])


def shards(echoes, triplet, bin_taper, phases, excluded, guard_len, train_len):
    bins, slots = triplet.shape
    chans = echoes.shape[2]
    span = slots * chans
    ranges = lax.axis_size("range")
    dops = lax.axis_size("dop")
    sizes = grid_sizes(ranges, dops)
    total_range = excluded.shape[1] * BLOCK * ranges
    own_gram = reduced_grams(triplet, echoes, excluded, sizes)
    owned = own_gram.shape[0] // span * 2
    owner = chunk_index(sizes, my_parts(sizes)) % (bins // owned)
    taper = lax.dynamic_slice_in_dim(bin_taper, owner * owned, owned, 0)
    turns = jnp.stack([jnp.cos(phases), jnp.sin(phases)])
    right = (taper[:, None, :, None] * turns[None, :, None, :]).reshape(2 * owned, span, 1)
    own_weights = solve(own_gram, right, total_range)
    weights = gather_weights(own_weights, sizes)
    power = apply_weights(triplet, echoes, weights, owned)
    padded = exchange_power(power, sizes)
    return detect(padded, guard_len, train_len, total_range)


def solution(mesh):
    placed = (
        P(None, None, None, ("range", "dop")),
        P(),
        P(),
        P(),
        P("dop", "range"),
        P("dop"),
        P("dop"),
    )
    return jax.shard_map(
        shards, mesh=mesh, in_specs=placed, out_specs=P("dop", "range"), check_vma=False
    )
```
